32 devices in a mesh: tm: 32 (over z, y, x, core).
Axes of the slice: x: 2, y: 2, z: 4, core: 2. Of those that a mesh axis runs over, the one named last changes fastest.
Arguments:
- samples: int32 [65536, 128], P('tm'), may hold values from -8 to 7
Outputs:
- spectra: float32 [2, 128, 16384], P(None, None, 'tm')
The draws below stay inside these ranges and needn't reach their ends.
All inputs are finite; a program needn't handle non-finite values.
Results may differ from the reference program's by a relative error of at most 0.0003.
Values may be sent and summed in bfloat16 or wider, within the bound.
A program may use at most 192 MiB of HBM per device.

```python
import jax
import jax.numpy as jnp
from jax import lax

INPUTS = 128
LAGS = 128
TOTAL = 65536


def plant(drawn, stream_key, least, high):
    shape = drawn.shape
    index_at = [jax.random.randint(jax.random.fold_in(stream_key, axis), (), 0, shape[axis]) for axis in range(len(shape))]
    drawn = drawn.at[tuple(index_at)].set(least)
    longest = shape.index(max(shape))
    index_at[longest] = (index_at[longest] + 1) % shape[longest]
    return drawn.at[tuple(index_at)].set(high)


def setup_inputs(seed: int = 0) -> dict:
    keys = jax.random.split(jax.random.key(seed), 2)
    samples = plant(jax.random.randint(keys[0], (TOTAL, INPUTS), -8, 8), jax.random.fold_in(keys[0], 1), -8, 7).astype(jnp.int32)
    return dict(samples=samples)


def reference(samples):
    values = samples.astype(jnp.float32)
    total = values.shape[0]
    width = values.shape[1]
    padded = jnp.concatenate([values, jnp.zeros((LAGS, width), jnp.float32)], axis=0)

    def one_lag(lag):
        window = lax.dynamic_slice(padded, (lag.astype(jnp.int32), jnp.int32(0)), (total, width))
        product = jnp.dot(window.T, values, preferred_element_type=jnp.float32, precision=lax.Precision.HIGHEST)
        return product.reshape(width * width)

    lagged = lax.map(one_lag, jnp.arange(LAGS, dtype=jnp.int32))
    lagged = lagged / (16.0 * total)
    transform = jnp.fft.fft(lagged, axis=0)
    return jnp.stack([jnp.real(transform), jnp.imag(transform)]).astype(jnp.float32)
```

```python
import functools

import jax
import jax.numpy as jnp
import numpy as np
from jax import lax
from jax.experimental import pallas as pl
from jax.experimental.pallas import tpu as pltpu
from jax.sharding import PartitionSpec as P

LAGS = 128
Q = 16
JS = 16
TAUS = LAGS + Q
OUT_ROWS = (LAGS + 1) * JS
TILE = OUT_ROWS // 3
MESH = pl.DeviceIdType.MESH


def flipped(value, mask):
    out = 0
    bit = 1
    while bit <= 64:
        b = (value // bit) % 2
        out = out + ((b + (1 if mask & bit else 0)) % 2) * bit
        bit *= 2
    return out


def kernel(n, T, G, mj, iw, samples, perm, out, vbuf, ts, tb, ut, acc, sbuf, rbuf,
           send_v, recv_v, send_t, recv_t, send_h, send_r, recv_r):
    me = lax.axis_index("tm")
    g = me % G
    t = me // G
    core = g % 2
    base = t * G
    rows = samples.shape[0]
    R = rows // Q
    C = G // 2

    for q in range(Q):
        phase = samples[pl.ds(q, R, stride=Q), :].astype(jnp.float32).astype(jnp.bfloat16)
        vbuf[g, q // 2, :, (q % 2) * 128:(q % 2 + 1) * 128] = phase
        turned = lax.dot_general(
            perm[...], phase, (((1,), (1,)), ((), ())), preferred_element_type=jnp.float32
        ).astype(jnp.bfloat16)
        for d in range(G):
            ts[d, q * JS:(q + 1) * JS, :] = turned[d * JS:(d + 1) * JS, :]

    def copy_t(k):
        d = flipped(g, k)
        return pltpu.make_async_remote_copy(
            src_ref=ts.at[d], dst_ref=tb.at[g], send_sem=send_t.at[k], recv_sem=recv_t.at[g],
            device_id=(base + d,), device_id_type=MESH)

    def copy_h(d):
        return pltpu.make_async_remote_copy(
            src_ref=ts.at[d], dst_ref=tb.at[G], send_sem=send_h.at[d], recv_sem=recv_t.at[G],
            device_id=(base - G + d,), device_id_type=MESH)

    def copy_v(slot, d, sem):
        return pltpu.make_async_remote_copy(
            src_ref=vbuf.at[slot], dst_ref=vbuf.at[slot], send_sem=send_v.at[sem],
            recv_sem=recv_v.at[slot], device_id=(base + d,), device_id_type=MESH)

    partner = flipped(g, 1)
    for k in range(1, G):
        copy_t(k).start()

    @pl.when(jnp.logical_and(g == 0, t > 0))
    def _():
        for d in range(G):
            copy_h(d).start()

    for c in range(1, C):
        copy_v(g, flipped(g, 2 * c), c).start()
    copy_v(g, partner, 0).start()

    tb[g] = ts[g]

    @pl.when(t == T - 1)
    def _():
        tb[G] = jnp.zeros(tb.shape[1:], tb.dtype)

    @pl.when(t < T - 1)
    def _():
        pltpu.make_async_copy(tb.at[G], tb.at[G], recv_t.at[G]).wait()

    for k in range(1, G):
        s = flipped(g, k)
        pltpu.make_async_copy(tb.at[s], tb.at[s], recv_t.at[s]).wait()

    def build(d, carry):
        pair = jnp.concatenate([tb[d], tb[d + 1]], axis=1)
        ut[d, 0:Q * JS, :] = tb[d]
        for s in range(1, TAUS // Q):
            ut[d, s * Q * JS:(s + 1) * Q * JS, :] = pair[:, s:s + R]
        return carry

    lax.fori_loop(0, G, build, 0)

    def multiply(d, first):
        weights = vbuf[d].reshape(Q // 2 * R, 256)

        def tile(i, carry):
            r0 = pl.multiple_of(i * TILE, JS)
            left = jnp.concatenate(
                [ut[d, pl.ds(pl.multiple_of(r0 + 2 * JS * e, JS), TILE), :] for e in range(Q // 2)], axis=1)
            part = jnp.dot(left, weights, preferred_element_type=jnp.float32)
            for h in range(2):
                half = part[:, h * 128:(h + 1) * 128]
                if first:
                    acc[h, pl.ds(r0, TILE), :] = half
                else:
                    acc[h, pl.ds(r0, TILE), :] += half
            return carry

        lax.fori_loop(0, OUT_ROWS // TILE, tile, 0)

    def wait_v(s):
        pltpu.make_async_copy(vbuf.at[s], vbuf.at[s], recv_v.at[s]).wait()

    multiply(g, True)
    wait_v(partner)
    multiply(partner, False)
    for c in range(1, C):
        s = flipped(g, 2 * c)
        wait_v(s)
        copy_v(s, partner, C + c - 1).start()
        multiply(s, False)
        if c > 1:
            s2 = flipped(g, 2 * (c - 1) + 1)
            wait_v(s2)
            multiply(s2, False)
    if C > 1:
        s2 = flipped(g, 2 * (C - 1) + 1)
        wait_v(s2)
        multiply(s2, False)

    def piece(j):
        full = acc[0, pl.ds(j, LAGS, stride=JS), :] + acc[1, pl.ds(JS + j, LAGS, stride=JS), :]
        if iw == 128:
            return full
        return sum(jnp.where(g % (128 // iw) == h, full[:, h * iw:(h + 1) * iw], 0.0) for h in range(128 // iw))

    def copy_r(k):
        d = (t + k) % T
        return pltpu.make_async_remote_copy(
            src_ref=sbuf.at[d], dst_ref=rbuf.at[t], send_sem=send_r.at[k], recv_sem=recv_r.at[t],
            device_id=(d * G + g,), device_id_type=MESH)

    for k in list(range(1, T)) + [0]:
        d = (t + k) % T
        for m in range(mj):
            if k:
                sbuf[d, m] = piece(d * mj + m)
            else:
                rbuf[t, m] = piece(d * mj + m)
        if k:
            copy_r(k).start()
    for k in range(1, T):
        s = (t + T - k) % T
        pltpu.make_async_copy(rbuf.at[s], rbuf.at[s], recv_r.at[s]).wait()
    for m in range(mj):
        total = rbuf[0, m]
        for k in range(1, T):
            total = total + rbuf[k, m]
        out[:, m * iw:(m + 1) * iw] = total

    for k in range(1, G):
        copy_t(k).wait_send()

    @pl.when(jnp.logical_and(g == 0, t > 0))
    def _():
        for d in range(G):
            copy_h(d).wait_send()

    for c in range(1, C):
        copy_v(g, flipped(g, 2 * c), c).wait_send()
        copy_v(flipped(g, 2 * c), partner, C + c - 1).wait_send()
    copy_v(g, partner, 0).wait_send()
    for k in range(1, T):
        copy_r(k).wait_send()


def on_device(n, samples):
    rows, width = samples.shape
    owned = width * width // n
    mj = max(1, owned // width)
    iw = min(width, owned)
    T = JS // mj
    G = n // T
    R = rows // Q
    perm = np.zeros((G * JS, width), np.float32)
    for d in range(G):
        for s in range(T):
            for m in range(mj):
                perm[d * JS + s * mj + m, (s * G + d) * owned // width + m] = 1
    lagged = pl.pallas_call(
        functools.partial(kernel, n, T, G, mj, iw),
        out_shape=jax.ShapeDtypeStruct((LAGS, owned), jnp.float32),
        in_specs=[pl.BlockSpec(memory_space=pltpu.VMEM)] * 2,
        out_specs=pl.BlockSpec(memory_space=pltpu.VMEM),
        scratch_shapes=[
            pltpu.VMEM((G, Q // 2, R, 2 * width), jnp.bfloat16),
            pltpu.VMEM((G, Q * JS, R), jnp.bfloat16),
            pltpu.VMEM((G + 1, Q * JS, R), jnp.bfloat16),
            pltpu.VMEM((G, TAUS * JS, R), jnp.bfloat16),
            pltpu.VMEM((2, OUT_ROWS, width), jnp.float32),
            pltpu.VMEM((T, mj, LAGS, iw), jnp.float32),
            pltpu.VMEM((T, mj, LAGS, iw), jnp.float32),
            pltpu.SemaphoreType.DMA((G,)),
            pltpu.SemaphoreType.DMA((G,)),
            pltpu.SemaphoreType.DMA((G,)),
            pltpu.SemaphoreType.DMA((G + 1,)),
            pltpu.SemaphoreType.DMA((G,)),
            pltpu.SemaphoreType.DMA((T,)),
            pltpu.SemaphoreType.DMA((T,)),
        ],
        compiler_params=pltpu.CompilerParams(has_side_effects=True, vmem_limit_bytes=56 * 1024 * 1024),
    )(samples, jnp.asarray(perm, jnp.bfloat16))
    k = np.arange(LAGS)
    angle = 2.0 * np.pi / LAGS * (np.outer(k, k) % LAGS)
    table = np.concatenate([np.cos(angle), -np.sin(angle)]) / (16.0 * rows * n)
    spectra = jnp.dot(
        jnp.asarray(table, jnp.float32), lagged,
        preferred_element_type=jnp.float32, precision=lax.Precision.HIGHEST)
    return spectra.reshape(2, LAGS, owned)


def solution(mesh):
    return jax.shard_map(
        functools.partial(on_device, mesh.shape["tm"]), mesh=mesh,
        in_specs=(P("tm", None),), out_specs=P(None, None, "tm"), check_vma=False)
```

```python
import functools

import jax
import jax.numpy as jnp
import numpy as np
from jax import lax
from jax.experimental import pallas as pl
from jax.experimental.pallas import tpu as pltpu
from jax.sharding import PartitionSpec as P

LAGS = 128
Q = 16
JS = 16
TAUS = LAGS + Q
OUT_ROWS = (LAGS + 1) * JS
TILE = OUT_ROWS // 3
MESH = pl.DeviceIdType.MESH


def flipped(value, mask):
    out = 0
    bit = 1
    while bit <= 64:
        b = (value // bit) % 2
        out = out + ((b + (1 if mask & bit else 0)) % 2) * bit
        bit *= 2
    return out


def code_levels(limit):
    for m in range(8192, 128, -128):
        steps = [m * e + limit / 2**e for e in range(20)]
        if min(steps) <= 32700:
            return m, int(np.argmin(steps)) + 1


def encoded(value, m, levels):
    size = jnp.abs(value)
    code = size
    for e in range(1, levels):
        code = jnp.minimum(code, size * 0.5**e + float(m * e))
    code = (code + 0.5).astype(jnp.int32)
    return jnp.where(value < 0, -code, code).astype(jnp.int16)


def decoded(code, m, levels):
    code = code.astype(jnp.int32).astype(jnp.float32)
    size = jnp.abs(code)
    value = size
    for e in range(1, levels):
        value = jnp.maximum(value, (size - float(m * e)) * 2.0**e)
    return jnp.where(code < 0, -value, value)


def kernel(n, T, G, mj, iw, samples, perm, out, vbuf, ts, tb, ut, acc, sbuf, rbuf,
           send_v, recv_v, send_t, recv_t, send_h, send_r, recv_r):
    me = lax.axis_index("tm")
    g = me % G
    t = me // G
    core = g % 2
    base = t * G
    rows = samples.shape[0]
    R = rows // Q
    C = G // 2
    half = Q // 4
    m_code, levels = code_levels(rows * G * 64)

    for q in range(Q):
        phase = samples[pl.ds(q, R, stride=Q), :].astype(jnp.float32).astype(jnp.bfloat16)
        vbuf[g, q // 2, :, (q % 2) * 128:(q % 2 + 1) * 128] = phase
        turned = lax.dot_general(
            perm[...], phase, (((1,), (1,)), ((), ())), preferred_element_type=jnp.float32
        ).astype(jnp.bfloat16)
        for d in range(G):
            ts[d, q * JS:(q + 1) * JS, :] = turned[d * JS:(d + 1) * JS, :]

    def copy_t(k):
        d = flipped(g, k)
        return pltpu.make_async_remote_copy(
            src_ref=ts.at[d], dst_ref=tb.at[g], send_sem=send_t.at[k], recv_sem=recv_t.at[g],
            device_id=(base + d,), device_id_type=MESH)

    def copy_h(d):
        return pltpu.make_async_remote_copy(
            src_ref=ts.at[d], dst_ref=tb.at[G], send_sem=send_h.at[d], recv_sem=recv_t.at[G],
            device_id=(base - G + d,), device_id_type=MESH)

    def copy_v(slot, d, h, sem):
        part = vbuf.at[slot, pl.ds(h * half, half)]
        return pltpu.make_async_remote_copy(
            src_ref=part, dst_ref=part, send_sem=send_v.at[sem, h],
            recv_sem=recv_v.at[slot, h], device_id=(base + d,), device_id_type=MESH)

    partner = flipped(g, 1)
    for k in range(1, G):
        copy_t(k).start()

    @pl.when(jnp.logical_and(g == 0, t > 0))
    def _():
        for d in range(G):
            copy_h(d).start()

    relay = C == 4
    sends = []

    def send(*what):
        copy_v(*what).start()
        sends.append(what)

    if relay:
        for k in range(2):
            send(g, flipped(g, 2), 1 - k, 1)
            send(g, flipped(g, 4), k, 2)
    else:
        for c in range(1, C):
            for h in range(2):
                send(g, flipped(g, 2 * c), h, c)
    for h in range(2):
        send(g, partner, h, 0)

    tb[g] = ts[g]

    @pl.when(t == T - 1)
    def _():
        tb[G] = jnp.zeros(tb.shape[1:], tb.dtype)

    @pl.when(t < T - 1)
    def _():
        pltpu.make_async_copy(tb.at[G], tb.at[G], recv_t.at[G]).wait()

    for k in range(1, G):
        s = flipped(g, k)
        pltpu.make_async_copy(tb.at[s], tb.at[s], recv_t.at[s]).wait()

    def build(d, carry):
        pair = jnp.concatenate([tb[d], tb[d + 1]], axis=1)
        ut[d, 0:Q * JS, :] = tb[d]
        for s in range(1, TAUS // Q):
            ut[d, s * Q * JS:(s + 1) * Q * JS, :] = pair[:, s:s + R]
        return carry

    lax.fori_loop(0, G, build, 0)

    def multiply(d, first):
        weights = vbuf[d].reshape(Q // 2 * R, 256)

        def tile(i, carry):
            r0 = pl.multiple_of(i * TILE, JS)
            left = jnp.concatenate(
                [ut[d, pl.ds(pl.multiple_of(r0 + 2 * JS * e, JS), TILE), :] for e in range(Q // 2)], axis=1)
            part = jnp.dot(left, weights, preferred_element_type=jnp.float32)
            for h in range(2):
                half = part[:, h * 128:(h + 1) * 128]
                if first:
                    acc[h, pl.ds(r0, TILE), :] = half
                else:
                    acc[h, pl.ds(r0, TILE), :] += half
            return carry

        lax.fori_loop(0, OUT_ROWS // TILE, tile, 0)

    def wait_v(s, h):
        part = vbuf.at[s, pl.ds(h * half, half)]
        pltpu.make_async_copy(part, part, recv_v.at[s, h]).wait()

    def wait_both(s):
        wait_v(s, 0)
        wait_v(s, 1)

    multiply(g, True)
    wait_both(partner)
    multiply(partner, False)
    if relay:
        x, y, z = (flipped(g, mask) for mask in (2, 4, 6))
        wait_v(x, 1)
        send(x, y, 1, 3)
        wait_v(y, 0)
        send(y, x, 0, 3)
        send(x, partner, 1, 4)
        send(y, partner, 0, 5)
        wait_v(x, 0)
        send(x, partner, 0, 4)
        wait_v(y, 1)
        send(y, partner, 1, 5)
        multiply(x, False)
        multiply(y, False)
        for mask in (3, 5):
            wait_both(flipped(g, mask))
            multiply(flipped(g, mask), False)
        for h in range(2):
            wait_v(z, h)
            send(z, partner, h, 6)
        multiply(z, False)
        wait_both(flipped(g, 7))
        multiply(flipped(g, 7), False)
    else:
        for c in range(1, C):
            s = flipped(g, 2 * c)
            for h in range(2):
                wait_v(s, h)
                send(s, partner, h, C + c - 1)
            multiply(s, False)
            if c > 1:
                s2 = flipped(g, 2 * (c - 1) + 1)
                wait_both(s2)
                multiply(s2, False)
        if C > 1:
            s2 = flipped(g, 2 * (C - 1) + 1)
            wait_both(s2)
            multiply(s2, False)

    def piece(j):
        full = acc[0, pl.ds(j, LAGS, stride=JS), :] + acc[1, pl.ds(JS + j, LAGS, stride=JS), :]
        if iw == 128:
            return full
        return sum(jnp.where(g % (128 // iw) == h, full[:, h * iw:(h + 1) * iw], 0.0) for h in range(128 // iw))

    def copy_r(k):
        d = (t + k) % T
        return pltpu.make_async_remote_copy(
            src_ref=sbuf.at[d], dst_ref=rbuf.at[t], send_sem=send_r.at[k], recv_sem=recv_r.at[t],
            device_id=(d * G + g,), device_id_type=MESH)

    for k in list(range(1, T)) + [0]:
        d = (t + k) % T
        for m in range(mj):
            if k:
                sbuf[d, m] = encoded(piece(d * mj + m), m_code, levels)
            else:
                out[:, m * iw:(m + 1) * iw] = piece(d * mj + m)
        if k:
            copy_r(k).start()
    for k in range(1, T):
        s = (t + T - k) % T
        pltpu.make_async_copy(rbuf.at[s], rbuf.at[s], recv_r.at[s]).wait()
        for m in range(mj):
            out[:, m * iw:(m + 1) * iw] += decoded(rbuf[s, m], m_code, levels)

    for k in range(1, G):
        copy_t(k).wait_send()

    @pl.when(jnp.logical_and(g == 0, t > 0))
    def _():
        for d in range(G):
            copy_h(d).wait_send()

    for what in sends:
        copy_v(*what).wait_send()
    for k in range(1, T):
        copy_r(k).wait_send()


def on_device(n, samples):
    rows, width = samples.shape
    owned = width * width // n
    mj = max(1, owned // width)
    iw = min(width, owned)
    T = JS // mj
    G = n // T
    R = rows // Q
    perm = np.zeros((G * JS, width), np.float32)
    for d in range(G):
        for s in range(T):
            for m in range(mj):
                perm[d * JS + s * mj + m, (s * G + d) * owned // width + m] = 1
    lagged = pl.pallas_call(
        functools.partial(kernel, n, T, G, mj, iw),
        out_shape=jax.ShapeDtypeStruct((LAGS, owned), jnp.float32),
        in_specs=[pl.BlockSpec(memory_space=pltpu.VMEM)] * 2,
        out_specs=pl.BlockSpec(memory_space=pltpu.VMEM),
        scratch_shapes=[
            pltpu.VMEM((G, Q // 2, R, 2 * width), jnp.bfloat16),
            pltpu.VMEM((G, Q * JS, R), jnp.bfloat16),
            pltpu.VMEM((G + 1, Q * JS, R), jnp.bfloat16),
            pltpu.VMEM((G, TAUS * JS, R), jnp.bfloat16),
            pltpu.VMEM((2, OUT_ROWS, width), jnp.float32),
            pltpu.VMEM((T, mj, LAGS, iw), jnp.int16),
            pltpu.VMEM((T, mj, LAGS, iw), jnp.int16),
            pltpu.SemaphoreType.DMA((G, 2)),
            pltpu.SemaphoreType.DMA((G, 2)),
            pltpu.SemaphoreType.DMA((G,)),
            pltpu.SemaphoreType.DMA((G + 1,)),
            pltpu.SemaphoreType.DMA((G,)),
            pltpu.SemaphoreType.DMA((T,)),
            pltpu.SemaphoreType.DMA((T,)),
        ],
        compiler_params=pltpu.CompilerParams(has_side_effects=True, vmem_limit_bytes=56 * 1024 * 1024),
    )(samples, jnp.asarray(perm, jnp.bfloat16))
    k = np.arange(LAGS)
    angle = 2.0 * np.pi / LAGS * (np.outer(k, k) % LAGS)
    table = np.concatenate([np.cos(angle), -np.sin(angle)]) / (16.0 * rows * n)
    spectra = jnp.dot(
        jnp.asarray(table, jnp.float32), lagged,
        preferred_element_type=jnp.float32, precision=lax.Precision.HIGHEST)
    return spectra.reshape(2, LAGS, owned)


def solution(mesh):
    return jax.shard_map(
        functools.partial(on_device, mesh.shape["tm"]), mesh=mesh,
        in_specs=(P("tm", None),), out_specs=P(None, None, "tm"), check_vma=False)
```

```python
import functools

import jax
import jax.numpy as jnp
import numpy as np
from jax import lax
from jax.experimental import pallas as pl
from jax.experimental.pallas import tpu as pltpu
from jax.sharding import PartitionSpec as P

LAGS = 128
Q = 16
JS = 16
TAUS = LAGS + Q
OUT_ROWS = (LAGS + 1) * JS
TILE = OUT_ROWS // 3
MESH = pl.DeviceIdType.MESH


def flipped(value, mask):
    out = 0
    bit = 1
    while bit <= 64:
        b = (value // bit) % 2
        out = out + ((b + (1 if mask & bit else 0)) % 2) * bit
        bit *= 2
    return out


def code_levels(limit):
    for m in range(8192, 128, -128):
        steps = [m * e + limit / 2**e for e in range(20)]
        if min(steps) <= 32700:
            return m, int(np.argmin(steps)) + 1


def encoded(value, m, levels):
    size = jnp.abs(value)
    code = size
    for e in range(1, levels):
        code = jnp.minimum(code, size * 0.5**e + float(m * e))
    code = (code + 0.5).astype(jnp.int32)
    return jnp.where(value < 0, -code, code).astype(jnp.int16)


def decoded(code, m, levels):
    code = code.astype(jnp.int32).astype(jnp.float32)
    size = jnp.abs(code)
    value = size
    for e in range(1, levels):
        value = jnp.maximum(value, (size - float(m * e)) * 2.0**e)
    return jnp.where(code < 0, -value, value)


def kernel(n, T, G, mj, iw, samples, perm, out, vbuf, ts, tb, ut, acc, sbuf, rbuf,
           send_v, recv_v, send_t, recv_t, send_h, send_r, recv_r):
    me = lax.axis_index("tm")
    g = me % G
    t = me // G
    core = g % 2
    base = t * G
    rows = samples.shape[0]
    R = rows // Q
    C = G // 2
    half = Q // 4
    m_code, levels = code_levels(rows * G * 64)

    barrier = pltpu.get_barrier_semaphore()

    def greet(device):
        pl.semaphore_signal(barrier, inc=1, device_id=(device,), device_id_type=MESH)

    for k in range(1, G):
        greet(base + flipped(g, k))
    for k in range(1, T):
        greet((t + k) % T * G + g)

    @pl.when(t < T - 1)
    def _():
        greet(base + G)

    for q in range(Q):
        phase = samples[pl.ds(q, R, stride=Q), :].astype(jnp.float32).astype(jnp.bfloat16)
        vbuf[g, q // 2, :, (q % 2) * 128:(q % 2 + 1) * 128] = phase

    feeds = jnp.logical_and(g == 0, t > 0)
    pl.semaphore_wait(barrier, jnp.where(feeds, 2 * G + T - 2, G + T - 2))

    def copy_t(k):
        d = flipped(g, k)
        return pltpu.make_async_remote_copy(
            src_ref=ts.at[d], dst_ref=tb.at[g], send_sem=send_t.at[k], recv_sem=recv_t.at[g],
            device_id=(base + d,), device_id_type=MESH)

    def copy_h(d):
        return pltpu.make_async_remote_copy(
            src_ref=ts.at[d], dst_ref=tb.at[G], send_sem=send_h.at[d], recv_sem=recv_t.at[G],
            device_id=(base - G + d,), device_id_type=MESH)

    def copy_v(slot, d, h, sem):
        part = vbuf.at[slot, pl.ds(h * half, half)]
        return pltpu.make_async_remote_copy(
            src_ref=part, dst_ref=part, send_sem=send_v.at[sem, h],
            recv_sem=recv_v.at[slot, h], device_id=(base + d,), device_id_type=MESH)

    partner = flipped(g, 1)
    relay = C == 4
    sends = []

    def send(*what):
        copy_v(*what).start()
        sends.append(what)

    if relay:
        send(g, flipped(g, 2), 1, 1)
        send(g, flipped(g, 4), 0, 2)

    for q in range(Q):
        turned = lax.dot_general(
            perm[...], vbuf[g, q // 2, :, (q % 2) * 128:(q % 2 + 1) * 128],
            (((1,), (1,)), ((), ())), preferred_element_type=jnp.float32
        ).astype(jnp.bfloat16)
        for d in range(G):
            ts[d, q * JS:(q + 1) * JS, :] = turned[d * JS:(d + 1) * JS, :]

    for k in range(G - 1, 0, -1):
        copy_t(k).start()

    @pl.when(jnp.logical_and(g == 0, t > 0))
    def _():
        for d in range(G):
            copy_h(d).start()

    if relay:
        send(g, flipped(g, 2), 0, 1)
        send(g, flipped(g, 4), 1, 2)
    else:
        for c in range(1, C):
            for h in range(2):
                send(g, flipped(g, 2 * c), h, c)
    for h in range(2):
        send(g, partner, h, 0)

    tb[g] = ts[g]

    @pl.when(t == T - 1)
    def _():
        tb[G] = jnp.zeros(tb.shape[1:], tb.dtype)

    @pl.when(t < T - 1)
    def _():
        pltpu.make_async_copy(tb.at[G], tb.at[G], recv_t.at[G]).wait()

    for k in range(1, G):
        s = flipped(g, k)
        pltpu.make_async_copy(tb.at[s], tb.at[s], recv_t.at[s]).wait()

    def build(d, carry):
        pair = jnp.concatenate([tb[d], tb[d + 1]], axis=1)
        ut[d, 0:Q * JS, :] = tb[d]
        for s in range(1, TAUS // Q):
            ut[d, s * Q * JS:(s + 1) * Q * JS, :] = pair[:, s:s + R]
        return carry

    lax.fori_loop(0, G, build, 0)

    def multiply(d, first):
        weights = vbuf[d].reshape(Q // 2 * R, 256)

        def tile(i, carry):
            r0 = pl.multiple_of(i * TILE, JS)
            left = jnp.concatenate(
                [ut[d, pl.ds(pl.multiple_of(r0 + 2 * JS * e, JS), TILE), :] for e in range(Q // 2)], axis=1)
            part = jnp.dot(left, weights, preferred_element_type=jnp.float32)
            for h in range(2):
                half = part[:, h * 128:(h + 1) * 128]
                if first:
                    acc[h, pl.ds(r0, TILE), :] = half
                else:
                    acc[h, pl.ds(r0, TILE), :] += half
            return carry

        lax.fori_loop(0, OUT_ROWS // TILE, tile, 0)

    def wait_v(s, h):
        part = vbuf.at[s, pl.ds(h * half, half)]
        pltpu.make_async_copy(part, part, recv_v.at[s, h]).wait()

    def wait_both(s):
        wait_v(s, 0)
        wait_v(s, 1)

    multiply(g, True)
    wait_both(partner)
    multiply(partner, False)
    if relay:
        x, y, z = (flipped(g, mask) for mask in (2, 4, 6))
        wait_v(x, 1)
        send(x, y, 1, 3)
        wait_v(y, 0)
        send(y, x, 0, 3)
        send(x, partner, 1, 4)
        send(y, partner, 0, 5)
        wait_v(x, 0)
        send(x, partner, 0, 4)
        wait_v(y, 1)
        send(y, partner, 1, 5)
        multiply(x, False)
        multiply(y, False)
        for mask in (3, 5):
            wait_both(flipped(g, mask))
            multiply(flipped(g, mask), False)
        for h in range(2):
            wait_v(z, h)
            send(z, partner, h, 6)
        multiply(z, False)
        wait_both(flipped(g, 7))
        multiply(flipped(g, 7), False)
    else:
        for c in range(1, C):
            s = flipped(g, 2 * c)
            for h in range(2):
                wait_v(s, h)
                send(s, partner, h, C + c - 1)
            multiply(s, False)
            if c > 1:
                s2 = flipped(g, 2 * (c - 1) + 1)
                wait_both(s2)
                multiply(s2, False)
        if C > 1:
            s2 = flipped(g, 2 * (C - 1) + 1)
            wait_both(s2)
            multiply(s2, False)

    def piece(j):
        full = acc[0, pl.ds(j, LAGS, stride=JS), :] + acc[1, pl.ds(JS + j, LAGS, stride=JS), :]
        if iw == 128:
            return full
        return sum(jnp.where(g % (128 // iw) == h, full[:, h * iw:(h + 1) * iw], 0.0) for h in range(128 // iw))

    def copy_r(k):
        d = (t + k) % T
        return pltpu.make_async_remote_copy(
            src_ref=sbuf.at[d], dst_ref=rbuf.at[t], send_sem=send_r.at[k], recv_sem=recv_r.at[t],
            device_id=(d * G + g,), device_id_type=MESH)

    for k in list(range(1, T)) + [0]:
        d = (t + k) % T
        for m in range(mj):
            if k:
                sbuf[d, m] = encoded(piece(d * mj + m), m_code, levels)
            else:
                out[:, m * iw:(m + 1) * iw] = piece(d * mj + m)
        if k:
            copy_r(k).start()
    for k in range(1, T):
        s = (t + T - k) % T
        pltpu.make_async_copy(rbuf.at[s], rbuf.at[s], recv_r.at[s]).wait()
        for m in range(mj):
            out[:, m * iw:(m + 1) * iw] += decoded(rbuf[s, m], m_code, levels)

    for k in range(1, G):
        copy_t(k).wait_send()

    @pl.when(jnp.logical_and(g == 0, t > 0))
    def _():
        for d in range(G):
            copy_h(d).wait_send()

    for what in sends:
        copy_v(*what).wait_send()
    for k in range(1, T):
        copy_r(k).wait_send()


def on_device(n, samples):
    rows, width = samples.shape
    owned = width * width // n
    mj = max(1, owned // width)
    iw = min(width, owned)
    T = JS // mj
    G = n // T
    R = rows // Q
    perm = np.zeros((G * JS, width), np.float32)
    for d in range(G):
        for s in range(T):
            for m in range(mj):
                perm[d * JS + s * mj + m, (s * G + d) * owned // width + m] = 1
    lagged = pl.pallas_call(
        functools.partial(kernel, n, T, G, mj, iw),
        out_shape=jax.ShapeDtypeStruct((LAGS, owned), jnp.float32),
        in_specs=[pl.BlockSpec(memory_space=pltpu.VMEM)] * 2,
        out_specs=pl.BlockSpec(memory_space=pltpu.VMEM),
        scratch_shapes=[
            pltpu.VMEM((G, Q // 2, R, 2 * width), jnp.bfloat16),
            pltpu.VMEM((G, Q * JS, R), jnp.bfloat16),
            pltpu.VMEM((G + 1, Q * JS, R), jnp.bfloat16),
            pltpu.VMEM((G, TAUS * JS, R), jnp.bfloat16),
            pltpu.VMEM((2, OUT_ROWS, width), jnp.float32),
            pltpu.VMEM((T, mj, LAGS, iw), jnp.int16),
            pltpu.VMEM((T, mj, LAGS, iw), jnp.int16),
            pltpu.SemaphoreType.DMA((G, 2)),
            pltpu.SemaphoreType.DMA((G, 2)),
            pltpu.SemaphoreType.DMA((G,)),
            pltpu.SemaphoreType.DMA((G + 1,)),
            pltpu.SemaphoreType.DMA((G,)),
            pltpu.SemaphoreType.DMA((T,)),
            pltpu.SemaphoreType.DMA((T,)),
        ],
        compiler_params=pltpu.CompilerParams(has_side_effects=True, collective_id=0, vmem_limit_bytes=56 * 1024 * 1024),
    )(samples, jnp.asarray(perm, jnp.bfloat16))
    k = np.arange(LAGS)
    angle = 2.0 * np.pi / LAGS * (np.outer(k, k) % LAGS)
    table = np.concatenate([np.cos(angle), -np.sin(angle)]) / (16.0 * rows * n)
    spectra = jnp.dot(
        jnp.asarray(table, jnp.float32), lagged,
        preferred_element_type=jnp.float32, precision=lax.Precision.HIGH)
    return spectra.reshape(2, LAGS, owned)


def solution(mesh):
    return jax.shard_map(
        functools.partial(on_device, mesh.shape["tm"]), mesh=mesh,
        in_specs=(P("tm", None),), out_specs=P(None, None, "tm"), check_vma=False)
```
